8 devices in a mesh: dp: 1 (over z), tp: 8 (over x, y, core).
Axes of the slice: x: 2, y: 2, z: 1, core: 2. Of those that a mesh axis runs over, the one named last changes fastest.
Arguments:
- x: bfloat16 [2048, 2560], P('dp')
- dy: bfloat16 [2048, 2560], P('dp')
- gate: bfloat16 [2048, 10240], P('dp', 'tp')
- up: bfloat16 [2048, 10240], P('dp', 'tp')
- w_gate: bfloat16 [2560, 10240], P(None, 'tp')
- w_up: bfloat16 [2560, 10240], P(None, 'tp')
- w_down: bfloat16 [10240, 2560], P('tp')
Outputs:
- output 1: bfloat16 [2048, 2560], P('dp')
- output 2: bfloat16 [2560, 10240], P('dp', 'tp')
- output 3: bfloat16 [2560, 10240], P('dp', 'tp')
- output 4: bfloat16 [10240, 2560], P(('dp', 'tp'))
All inputs are finite; a program needn't handle non-finite values.
Results may differ from the reference program's by a relative error of at most 0.012.
Values are sent between devices in bfloat16 or wider.
A program may use at most 2 GiB of HBM per device.

```python
import jax
import jax.numpy as jnp

ROWS = 2048
D = 2560
FF = 10240


def act(gate, up):
    return jax.nn.gelu(gate) * up


def setup_inputs(seed: int = 0, part: int = 0) -> dict:
    kx, ky, ka, kb, kg, ku, kd = jax.random.split(jax.random.key(seed), 7)
    kx, ky, ka, kb = (jax.random.fold_in(k, part) for k in (kx, ky, ka, kb))
    drawn = {
        "x": jax.random.normal(kx, (ROWS, D), jnp.float32),
        "dy": jax.random.normal(ky, (ROWS, D), jnp.float32),
        "gate": jax.random.normal(ka, (ROWS, FF), jnp.float32),
        "up": jax.random.normal(kb, (ROWS, FF), jnp.float32),
        "w_gate": jax.random.normal(kg, (D, FF), jnp.float32) * D**-0.5,
        "w_up": jax.random.normal(ku, (D, FF), jnp.float32) * D**-0.5,
        "w_down": jax.random.normal(kd, (FF, D), jnp.float32) * FF**-0.5,
    }
    return {k: v.astype(jnp.bfloat16) for k, v in drawn.items()}


def reference(x, dy, gate, up, w_gate, w_up, w_down):
    hidden, back = jax.vjp(act, gate.astype(jnp.float32), up.astype(jnp.float32))
    d_hidden = jnp.dot(dy, w_down.T, preferred_element_type=jnp.float32)
    d_gate, d_up = (g.astype(jnp.bfloat16) for g in back(d_hidden))
    dx = jnp.dot(d_gate, w_gate.T, preferred_element_type=jnp.float32) + jnp.dot(d_up, w_up.T, preferred_element_type=jnp.float32)
    dw_gate = jnp.dot(x.T, d_gate, preferred_element_type=jnp.float32)
    dw_up = jnp.dot(x.T, d_up, preferred_element_type=jnp.float32)
    dw_down = jnp.dot(hidden.astype(jnp.bfloat16).T, dy, preferred_element_type=jnp.float32)
    return tuple(g.astype(jnp.bfloat16) for g in (dx, dw_gate, dw_up, dw_down))
```

```python
import jax
import jax.numpy as jnp
from jax import lax
from jax.experimental import pallas as pl
from jax.experimental.pallas import tpu as pltpu
from jax.sharding import PartitionSpec as P

MESH = pl.DeviceIdType.MESH
BF16, F32 = jnp.bfloat16, jnp.float32
SQRT_2_OVER_PI = 0.7978845608028654
CUBIC = 0.044715

T, D, F = 2048, 2560, 1280
N = 8
R = T // N
S = R // 2
Q = R // 4
H = D // 2
NT = 256
SLOTS = 4
STAGES = ("pair", "a", "b", "c", "own", "fwd", "e1", "e2")

TICKS = {
    "a": (7, 11, 15, 17, 24, 28, 35, 40),
    "b": (10, 15, 18, 21, 28, 32, 39, 45),
    "c": (13, 20, 23, 25, 34, 37, 43, 49),
    "d": (19, 29, 37, 42, 47, 49, 52, 54),
}


def dot_nt(a, b):
    return lax.dot_general(a, b, (((1,), (1,)), ((), ())), preferred_element_type=F32)


def kernel(x, dy, gate, up, wg, wu, wd, dx, dwg, dwu, dwd, dg, du, ht, dyb, xt, acc, pair_in, a_in, b_in, pair_out, a_out, b_out, w_sem, in_sem, x_sem, send_sem, recv_sem, free_sem):
    me = lax.axis_index("tp")
    core = lax.rem(me, 2)
    px, py = me // 4, lax.rem(me // 2, 2)
    p = jnp.where(core == 0, px, py)
    s = jnp.where(core == 0, py, px)
    over_x = (1 - px) * 4 + py * 2 + core
    over_y = px * 4 + (1 - py) * 2 + core
    n1 = jnp.where(core == 0, over_x, over_y)
    n2 = jnp.where(core == 0, over_y, over_x)
    partner = px * 4 + py * 2 + (1 - core)

    mine = pl.ds(pl.multiple_of(core * H, H), H)

    def rows(j, start, size):
        return pl.ds(pl.multiple_of(j * R + start, Q), size)

    def remote(stage, j, src, dst, to):
        k = STAGES.index(stage)
        return pltpu.make_async_remote_copy(src, dst, send_sem.at[k, j], recv_sem.at[k, j], device_id={"tp": to}, device_id_type=MESH)

    def copy_of(stage, j):
        if stage == "pair":
            return remote(stage, j, pair_out.at[lax.rem(j, 2)], pair_in.at[lax.rem(j, 2)], partner)
        if stage == "a":
            return remote(stage, j, a_out.at[lax.rem(j, SLOTS)], a_in.at[lax.rem(j, SLOTS)], n1)
        if stage == "b":
            return remote(stage, j, b_out.at[lax.rem(j, SLOTS)], b_in.at[j], n2)
        if stage == "c":
            at = dx.at[rows(j, S * p + Q * s, Q), mine]
            return remote(stage, j, at, at, n2)
        if stage == "own":
            at = dx.at[rows(j, S * p + Q * s, Q), mine]
            return remote(stage, j, at, at, n1)
        if stage == "fwd":
            at = dx.at[rows(j, S * p + Q * (1 - s), Q), mine]
            return remote(stage, j, at, at, n1)
        at = dx.at[rows(j, S * p if stage == "e1" else S * (1 - p), S), mine]
        return remote(stage, j, at, at, partner)

    def reuse(stage, j, slots):
        @pl.when(j >= slots)
        def _():
            copy_of(stage, j - slots).wait_send()

    def take_a(j):
        copy_of("a", j).wait_recv()
        reuse("b", j, SLOTS)
        k = lax.rem(j, SLOTS)
        keep, leave = pl.ds(pl.multiple_of(Q * s, Q), Q), pl.ds(pl.multiple_of(Q * (1 - s), Q), Q)
        b_out[k] = (acc[k, leave, :] + a_in[k, leave, :].astype(F32)).astype(BF16)
        copy_of("b", j).start()
        acc[k, keep, :] = acc[k, keep, :] + a_in[k, keep, :].astype(F32)

        @pl.when(j + SLOTS < N)
        def _():
            pl.semaphore_signal(free_sem, inc=1, device_id={"tp": n1}, device_id_type=MESH)

    def take_b(j):
        copy_of("b", j).wait_recv()
        keep = pl.ds(pl.multiple_of(Q * s, Q), Q)
        dx[rows(j, S * p + Q * s, Q), mine] = (acc[lax.rem(j, SLOTS), keep, :] + b_in[j].astype(F32)).astype(BF16)
        copy_of("c", j).start()
        copy_of("own", j).start()

    def take_c(j):
        copy_of("c", j).wait_recv()
        copy_of("fwd", j).start()
        copy_of("e1", j).start()

    def take_d(j):
        copy_of("own", j).wait_recv()
        copy_of("fwd", j).wait_recv()
        copy_of("e2", j).start()

    def tick(t, first, last):
        for name, take in (("a", take_a), ("b", take_b), ("c", take_c), ("d", take_d)):
            due = [(j, at) for j, at in enumerate(TICKS[name]) if first <= at <= last]
            if due:
                hit = sum((t == at).astype(jnp.int32) for _, at in due)
                j = sum((t == at).astype(jnp.int32) * j for j, at in due)

                @pl.when(hit > 0)
                def _(take=take, j=j):
                    take(j)

    def local(src, dst, sem):
        return pltpu.make_async_copy(src, dst, sem)

    def inputs(i):
        at = pl.ds(pl.multiple_of(i * R, R), R)
        return (
            local(dy.at[at], dyb, in_sem.at[0]),
            local(gate.at[at], dg.at[at], in_sem.at[1]),
            local(up.at[at], du.at[at], in_sem.at[2]),
        )

    weights = [local(src, dst, w_sem.at[k]) for k, (src, dst) in enumerate(((wd, dwd), (wg, dwg), (wu, dwu)))]
    weights[0].start()
    for c in inputs(0):
        c.start()
    weights[1].start()
    weights[2].start()

    barrier = pltpu.get_barrier_semaphore()
    for other in (n1, n2, partner):
        pl.semaphore_signal(barrier, inc=1, device_id={"tp": other}, device_id_type=MESH)
    pl.semaphore_wait(barrier, 3)

    def hidden_part(i):
        at = pl.ds(pl.multiple_of(i * R, R), R)
        dyv = dyb[...]
        for n in range(F // NT):
            cols = pl.ds(n * NT, NT)
            d_hidden = dot_nt(dyv, dwd[cols, :])
            g, u = dg[at, cols].astype(F32), du[at, cols].astype(F32)
            g2 = g * g
            h = 0.5 + 0.5 * jnp.tanh(g * (SQRT_2_OVER_PI + (SQRT_2_OVER_PI * CUBIC) * g2))
            a = g * h
            slope = h + (g * (h - h * h)) * (2 * SQRT_2_OVER_PI + (6 * SQRT_2_OVER_PI * CUBIC) * g2)
            dg[at, cols] = ((d_hidden * u) * slope).astype(BF16)
            du[at, cols] = (d_hidden * a).astype(BF16)
            ht[cols, at] = (a * u).astype(BF16).T

    def term(j, n, col0):
        at = pl.ds(pl.multiple_of(j * R, R), R)
        w = pl.ds(pl.multiple_of(col0 + n * NT, NT), NT)
        d = jnp.concatenate([dg[at, :], du[at, :]], axis=1)
        return dot_nt(d, jnp.concatenate([dwg[w, :], dwu[w, :]], axis=1))

    def pair_part(j):
        reuse("pair", j, 2)
        slot = lax.rem(j, 2)
        for n in range(H // NT):
            pair_out[slot, :, pl.ds(n * NT, NT)] = term(j, n, (1 - core) * H).astype(BF16)
        copy_of("pair", j).start()

    def own_part(j):
        copy_of("pair", j).wait_recv()
        reuse("a", j, SLOTS)
        slot, k = lax.rem(j, 2), lax.rem(j, SLOTS)
        for n in range(H // NT):
            cols = pl.ds(n * NT, NT)
            acc_t = term(j, n, core * H)
            tmp = acc_t + pair_in[slot, :, cols].astype(F32)
            lo, hi = tmp[:S], tmp[S:]
            kept = jnp.where(p == 0, lo, hi)
            sent = jnp.where(p == 0, hi, lo)
            acc[k, :, cols] = kept
            a_out[k, :, cols] = sent.astype(BF16)

        @pl.when(j >= SLOTS)
        def _():
            pl.semaphore_wait(free_sem, 1)

        copy_of("a", j).start()

    def chunk(i, _):
        for c in inputs(i):
            c.wait()

        @pl.when(i == 0)
        def _():
            weights[0].wait()

        hidden_part(i)

        @pl.when(i + 1 < N)
        def _():
            for c in inputs(i + 1):
                c.start()

        tick(3 * i, 0, 3 * N - 1)

        @pl.when(i == 0)
        def _():
            weights[1].wait()
            weights[2].wait()

        @pl.when(i > 0)
        def _():
            own_part(i - 1)

        tick(3 * i + 1, 0, 3 * N - 1)
        pair_part(i)
        tick(3 * i + 2, 0, 3 * N - 1)
        return ()

    lax.fori_loop(0, N, chunk, ())

    def tile(src, n):
        slot = lax.rem(n, 2)
        return local(src.at[:, pl.ds(pl.multiple_of(n * NT, NT), NT)], xt.at[slot], x_sem.at[slot])

    TILES = D // NT
    tile(dy, 0).start()
    own_part(N - 1)
    t0 = 3 * N
    tick(jnp.int32(t0), t0, t0)
    t0 += 1

    def down(n, _):
        tile(dy, n).wait()

        @pl.when(n + 1 < TILES)
        def _():
            tile(dy, n + 1).start()

        @pl.when(n + 1 == TILES)
        def _():
            tile(x, jnp.int32(TILES - TILES)).start()

        cols = pl.ds(pl.multiple_of(n * NT, NT), NT)
        dwd[:, cols] = jnp.dot(ht[...], xt[lax.rem(n, 2)], preferred_element_type=F32).astype(BF16)
        tick(t0 + n, t0, t0 + TILES - 1)
        return ()

    lax.fori_loop(0, TILES, down, ())
    t1 = t0 + TILES

    def gate_up(n, _):
        tile(x, n).wait()

        @pl.when(n + 1 < TILES)
        def _():
            tile(x, n + 1).start()

        at = pl.ds(pl.multiple_of(n * NT, NT), NT)
        xv = xt[lax.rem(n, 2)].T
        dwg[at, :] = jnp.dot(xv, dg[...], preferred_element_type=F32).astype(BF16)
        tick(t1 + 2 * n, t1, t1 + 2 * TILES - 1)
        dwu[at, :] = jnp.dot(xv, du[...], preferred_element_type=F32).astype(BF16)
        tick(t1 + 2 * n + 1, t1, t1 + 2 * TILES - 1)
        return ()

    lax.fori_loop(0, TILES, gate_up, ())

    def finish(j, _):
        copy_of("e1", j).wait_recv()
        copy_of("e2", j).wait_recv()
        for stage in STAGES[3:]:
            copy_of(stage, j).wait_send()
        for stage, slots in (("pair", 2), ("a", SLOTS), ("b", SLOTS)):

            @pl.when(j >= N - slots)
            def _(stage=stage):
                copy_of(stage, j).wait_send()

        return ()

    lax.fori_loop(0, N, finish, ())


def store(*refs):
    n = (len(refs) - 1) // 2
    copies = [pltpu.make_async_copy(refs[k], refs[n + k], refs[-1].at[k]) for k in range(n)]
    for c in copies:
        c.start()
    for c in copies:
        c.wait()


def solution(mesh):
    def step(x, dy, gate, up, w_gate, w_up, w_down):
        hbm = pl.BlockSpec(memory_space=pltpu.HBM)
        vmem = pl.BlockSpec(memory_space=pltpu.VMEM)
        dma = pltpu.SemaphoreType.DMA
        held = pl.pallas_call(
            kernel,
            name="mlp_backward",
            in_specs=[hbm] * 7,
            out_specs=[vmem] * 4,
            out_shape=[pltpu.VMEM((T, D), BF16), pltpu.VMEM((D, F), BF16), pltpu.VMEM((D, F), BF16), pltpu.VMEM((F, D), BF16)],
            scratch_shapes=[
                pltpu.VMEM((T, F), BF16),
                pltpu.VMEM((T, F), BF16),
                pltpu.VMEM((F, T), BF16),
                pltpu.VMEM((R, D), BF16),
                pltpu.VMEM((2, T, NT), BF16),
                pltpu.VMEM((SLOTS, S, H), F32),
                pltpu.VMEM((2, R, H), BF16),
                pltpu.VMEM((SLOTS, S, H), BF16),
                pltpu.VMEM((N, Q, H), BF16),
                pltpu.VMEM((2, R, H), BF16),
                pltpu.VMEM((SLOTS, S, H), BF16),
                pltpu.VMEM((SLOTS, Q, H), BF16),
                dma((3,)),
                dma((3,)),
                dma((2,)),
                dma((len(STAGES), N)),
                dma((len(STAGES), N)),
                pltpu.SemaphoreType.REGULAR,
            ],
            compiler_params=pltpu.CompilerParams(collective_id=0, has_side_effects=True, vmem_limit_bytes=35 * 2**20),
            cost_estimate=pl.CostEstimate(flops=12 * T * D * F, bytes_accessed=80 * 2**20, transcendentals=T * F),
        )(x, dy, gate, up, w_gate, w_up, w_down)
        return pl.pallas_call(
            store,
            name="store",
            in_specs=[vmem] * 4,
            out_specs=[hbm] * 4,
            out_shape=[jax.ShapeDtypeStruct(h.shape, BF16) for h in held],
            scratch_shapes=[dma((4,))],
            compiler_params=pltpu.CompilerParams(vmem_limit_bytes=2**20),
        )(*held)

    tokens, columns, down = P("dp", None), P(None, "tp"), P("tp", None)
    return jax.shard_map(
        step,
        mesh=mesh,
        in_specs=(tokens, tokens, P("dp", "tp"), P("dp", "tp"), columns, columns, down),
        out_specs=(tokens, P("dp", "tp"), P("dp", "tp"), P(("dp", "tp"), None)),
        check_vma=False,
    )
```

```python
import jax
import jax.numpy as jnp
from jax import lax
from jax.experimental import pallas as pl
from jax.experimental.pallas import tpu as pltpu
from jax.sharding import PartitionSpec as P

MESH = pl.DeviceIdType.MESH
BF16, F32 = jnp.bfloat16, jnp.float32
SQRT_2_OVER_PI = 0.7978845608028654
CUBIC = 0.044715

T, D, F = 2048, 2560, 1280
N = 8
R = T // N
S = R // 2
Q = R // 4
H = D // 2
NT = 256
SLOTS = 4
STAGES = ("pair", "a", "b", "c", "own", "fwd", "e1", "e2")

TICKS = {
    "a": (0, 4, 11, 12, 18, 22, 28, 31),
    "b": (3, 8, 15, 17, 23, 27, 31, 34),
    "c": (6, 11, 20, 21, 29, 34, 35, 36),
    "d": (11, 20, 31, 34, 36, 43, 46, 47),
}


def dot_nt(a, b):
    return lax.dot_general(a, b, (((1,), (1,)), ((), ())), preferred_element_type=F32)


def kernel(x, dy, gate, up, wg, wu, wd, dx, dwg, dwu, dwd, dg, du, ht, dyb, xt, acc, pair_in, a_in, b_in, pair_out, a_out, b_out, w_sem, in_sem, x_sem, send_sem, recv_sem, free_sem):
    me = lax.axis_index("tp")
    core = lax.rem(me, 2)
    px, py = me // 4, lax.rem(me // 2, 2)
    p = jnp.where(core == 0, px, py)
    s = jnp.where(core == 0, py, px)
    over_x = (1 - px) * 4 + py * 2 + core
    over_y = px * 4 + (1 - py) * 2 + core
    n1 = jnp.where(core == 0, over_x, over_y)
    n2 = jnp.where(core == 0, over_y, over_x)
    partner = px * 4 + py * 2 + (1 - core)

    mine = pl.ds(pl.multiple_of(core * H, H), H)

    def rows(j, start, size):
        return pl.ds(pl.multiple_of(j * R + start, Q), size)

    def remote(stage, j, src, dst, to):
        k = STAGES.index(stage)
        return pltpu.make_async_remote_copy(src, dst, send_sem.at[k, j], recv_sem.at[k, j], device_id={"tp": to}, device_id_type=MESH)

    def copy_of(stage, j):
        if stage == "pair":
            return remote(stage, j, pair_out.at[lax.rem(j, 2)], pair_in.at[lax.rem(j, 2)], partner)
        if stage == "a":
            return remote(stage, j, a_out.at[lax.rem(j, SLOTS)], a_in.at[lax.rem(j, SLOTS)], n1)
        if stage == "b":
            return remote(stage, j, b_out.at[lax.rem(j, SLOTS)], b_in.at[j], n2)
        if stage == "c":
            at = dx.at[rows(j, S * p + Q * s, Q), mine]
            return remote(stage, j, at, at, n2)
        if stage == "own":
            at = dx.at[rows(j, S * p + Q * s, Q), mine]
            return remote(stage, j, at, at, n1)
        if stage == "fwd":
            at = dx.at[rows(j, S * p + Q * (1 - s), Q), mine]
            return remote(stage, j, at, at, n1)
        at = dx.at[rows(j, S * p if stage == "e1" else S * (1 - p), S), mine]
        return remote(stage, j, at, at, partner)

    def reuse(stage, j, slots):
        @pl.when(j >= slots)
        def _():
            copy_of(stage, j - slots).wait_send()

    def take_a(j):
        copy_of("a", j).wait_recv()
        reuse("b", j, SLOTS)
        k = lax.rem(j, SLOTS)
        keep, leave = pl.ds(pl.multiple_of(Q * s, Q), Q), pl.ds(pl.multiple_of(Q * (1 - s), Q), Q)
        b_out[k] = (acc[k, leave, :] + a_in[k, leave, :].astype(F32)).astype(BF16)
        copy_of("b", j).start()
        acc[k, keep, :] = acc[k, keep, :] + a_in[k, keep, :].astype(F32)

        @pl.when(j + SLOTS < N)
        def _():
            pl.semaphore_signal(free_sem, inc=1, device_id={"tp": n1}, device_id_type=MESH)

    def take_b(j):
        copy_of("b", j).wait_recv()
        keep = pl.ds(pl.multiple_of(Q * s, Q), Q)
        dx[rows(j, S * p + Q * s, Q), mine] = (acc[lax.rem(j, SLOTS), keep, :] + b_in[j].astype(F32)).astype(BF16)
        copy_of("c", j).start()
        copy_of("own", j).start()

    def take_c(j):
        copy_of("c", j).wait_recv()
        copy_of("fwd", j).start()
        copy_of("e1", j).start()

    def take_d(j):
        copy_of("own", j).wait_recv()
        copy_of("fwd", j).wait_recv()
        copy_of("e2", j).start()

    def tick(t, first, last):
        for name, take in (("a", take_a), ("b", take_b), ("c", take_c), ("d", take_d)):
            due = [(j, at) for j, at in enumerate(TICKS[name]) if first <= at <= last]
            if due:
                hit = sum((t == at).astype(jnp.int32) for _, at in due)
                j = sum((t == at).astype(jnp.int32) * j for j, at in due)

                @pl.when(hit > 0)
                def _(take=take, j=j):
                    take(j)

    def local(src, dst, sem):
        return pltpu.make_async_copy(src, dst, sem)

    def inputs(i):
        at = pl.ds(pl.multiple_of(i * R, R), R)
        return (
            local(dy.at[at], dyb, in_sem.at[0]),
            local(gate.at[at], dg.at[at], in_sem.at[1]),
            local(up.at[at], du.at[at], in_sem.at[2]),
        )

    def half(k):
        at = pl.ds(pl.multiple_of((1 - core if k == 0 else core) * H, H), H)
        return local(wg.at[at], dwg.at[at], w_sem.at[2 * k]), local(wu.at[at], dwu.at[at], w_sem.at[2 * k + 1])

    down_weight = local(wd, dwd, w_sem.at[4])
    down_weight.start()
    for c in (*inputs(0), *half(0), *half(1)):
        c.start()

    barrier = pltpu.get_barrier_semaphore()
    for other in (n1, n2, partner):
        pl.semaphore_signal(barrier, inc=1, device_id={"tp": other}, device_id_type=MESH)

    def hidden_part(i):
        at = pl.ds(pl.multiple_of(i * R, R), R)
        dyv = dyb[...]
        for n in range(F // NT):
            cols = pl.ds(n * NT, NT)
            d_hidden = dot_nt(dyv, dwd[cols, :])
            g, u = dg[at, cols].astype(F32), du[at, cols].astype(F32)
            g2 = g * g
            h = 0.5 + 0.5 * jnp.tanh(g * (SQRT_2_OVER_PI + (SQRT_2_OVER_PI * CUBIC) * g2))
            a = g * h
            slope = h + (g * (h - h * h)) * (2 * SQRT_2_OVER_PI + (6 * SQRT_2_OVER_PI * CUBIC) * g2)
            dg[at, cols] = ((d_hidden * u) * slope).astype(BF16)
            du[at, cols] = (d_hidden * a).astype(BF16)
            ht[cols, at] = (a * u).astype(BF16).T

    def term(j, n, col0):
        at = pl.ds(pl.multiple_of(j * R, R), R)
        w = pl.ds(pl.multiple_of(col0 + n * NT, NT), NT)
        d = jnp.concatenate([dg[at, :], du[at, :]], axis=1)
        return dot_nt(d, jnp.concatenate([dwg[w, :], dwu[w, :]], axis=1))

    def pair_part(j):
        reuse("pair", j, 2)
        slot = lax.rem(j, 2)
        for n in range(H // NT):
            pair_out[slot, :, pl.ds(n * NT, NT)] = term(j, n, (1 - core) * H).astype(BF16)
        copy_of("pair", j).start()

    def own_ready(j):
        copy_of("pair", j).wait_recv()
        reuse("a", j, SLOTS)

        @pl.when(j >= SLOTS)
        def _():
            pl.semaphore_wait(free_sem, 1)

    def own_part(j):
        slot, k = lax.rem(j, 2), lax.rem(j, SLOTS)
        for n in range(H // NT):
            cols = pl.ds(n * NT, NT)
            total = term(j, n, core * H) + pair_in[slot, :, cols].astype(F32)
            lo, hi = total[:S], total[S:]
            acc[k, :, cols] = jnp.where(p == 0, lo, hi)
            a_out[k, :, cols] = jnp.where(p == 0, hi, lo).astype(BF16)
        copy_of("a", j).start()

    def wait_inputs(i):
        for c in inputs(i):
            c.wait()

    def next_inputs(i):
        @pl.when(i < N)
        def _():
            for c in inputs(i):
                c.start()

    zero, one = jnp.int32(0), jnp.int32(1)

    def part(f, j):
        @pl.when(me >= 0)
        def _():
            f(j)

    wait_inputs(zero)
    down_weight.wait()
    part(hidden_part, zero)
    next_inputs(one)
    for c in half(0):
        c.wait()
    pl.semaphore_wait(barrier, 3)
    part(pair_part, zero)
    for c in half(1):
        c.wait()
    own_ready(zero)
    part(own_part, zero)
    wait_inputs(one)
    part(hidden_part, one)
    next_inputs(one + 1)
    part(pair_part, one)
    LAST = 3 * N - 7

    def chunk(i, _):
        wait_inputs(i)
        hidden_part(i)
        next_inputs(i + 1)
        tick(3 * i - 6, 0, LAST)
        own_ready(i - 1)

        @pl.when(i > 1)
        def _():
            own_part(i - 1)

        tick(3 * i - 5, 0, LAST)
        pair_part(i)
        tick(3 * i - 4, 0, LAST)
        return ()

    lax.fori_loop(2, N, chunk, ())

    def tile(src, n):
        slot = lax.rem(n, 2)
        return local(src.at[:, pl.ds(pl.multiple_of(n * NT, NT), NT)], xt.at[slot], x_sem.at[slot])

    TILES = D // NT
    tile(dy, 0).start()
    own_ready(jnp.int32(N - 1))
    own_part(jnp.int32(N - 1))
    t0 = LAST + 1
    tick(jnp.int32(t0), t0, t0)
    t0 += 1

    def down(n, _):
        tile(dy, n).wait()

        @pl.when(n + 1 < TILES)
        def _():
            tile(dy, n + 1).start()

        @pl.when(n + 1 == TILES)
        def _():
            tile(x, zero).start()

        cols = pl.ds(pl.multiple_of(n * NT, NT), NT)
        dwd[:, cols] = jnp.dot(ht[...], xt[lax.rem(n, 2)], preferred_element_type=F32).astype(BF16)
        tick(t0 + n, t0, t0 + TILES - 1)
        return ()

    lax.fori_loop(0, TILES, down, ())
    t1 = t0 + TILES

    def turn(n):
        ht[pl.ds(pl.multiple_of(lax.rem(n, 2) * NT, NT), NT), :] = xt[lax.rem(n, 2)].T

    tile(x, zero).wait()
    tile(x, one).start()
    turn(zero)

    def gate_up(n, _):
        @pl.when(n + 1 < TILES)
        def _():
            tile(x, n + 1).wait()

        @pl.when(n + 2 < TILES)
        def _():
            tile(x, n + 2).start()

        at = pl.ds(pl.multiple_of(n * NT, NT), NT)
        xv = ht[pl.ds(pl.multiple_of(lax.rem(n, 2) * NT, NT), NT), :]
        dwg[at, :] = jnp.dot(xv, dg[...], preferred_element_type=F32).astype(BF16)
        turn(n + 1)
        dwu[at, :] = jnp.dot(xv, du[...], preferred_element_type=F32).astype(BF16)
        tick(t1 + n, t1, t1 + TILES - 1)
        return ()

    lax.fori_loop(0, TILES, gate_up, ())

    t2 = t1 + TILES

    def drain(t, _):
        tick(t, t2, 99)
        return ()

    lax.fori_loop(t2, max(TICKS["d"]) + 1, drain, ())

    def finish(j, _):
        copy_of("e1", j).wait_recv()
        copy_of("e2", j).wait_recv()
        for stage in STAGES[3:]:
            copy_of(stage, j).wait_send()
        for stage, slots in (("pair", 2), ("a", SLOTS), ("b", SLOTS)):

            @pl.when(j >= N - slots)
            def _(stage=stage):
                copy_of(stage, j).wait_send()

        return ()

    lax.fori_loop(0, N, finish, ())


def store(*refs):
    n = (len(refs) - 1) // 2
    copies = [pltpu.make_async_copy(refs[k], refs[n + k], refs[-1].at[k]) for k in range(n)]
    for c in copies:
        c.start()
    for c in copies:
        c.wait()


def solution(mesh):
    def step(x, dy, gate, up, w_gate, w_up, w_down):
        hbm = pl.BlockSpec(memory_space=pltpu.HBM)
        vmem = pl.BlockSpec(memory_space=pltpu.VMEM)
        dma = pltpu.SemaphoreType.DMA
        held = pl.pallas_call(
            kernel,
            name="mlp_backward",
            in_specs=[hbm] * 7,
            out_specs=[vmem] * 4,
            out_shape=[pltpu.VMEM((T, D), BF16), pltpu.VMEM((D, F), BF16), pltpu.VMEM((D, F), BF16), pltpu.VMEM((F, D), BF16)],
            scratch_shapes=[
                pltpu.VMEM((T, F), BF16),
                pltpu.VMEM((T, F), BF16),
                pltpu.VMEM((F, T), BF16),
                pltpu.VMEM((R, D), BF16),
                pltpu.VMEM((2, T, NT), BF16),
                pltpu.VMEM((SLOTS, S, H), F32),
                pltpu.VMEM((2, R, H), BF16),
                pltpu.VMEM((SLOTS, S, H), BF16),
                pltpu.VMEM((N, Q, H), BF16),
                pltpu.VMEM((2, R, H), BF16),
                pltpu.VMEM((SLOTS, S, H), BF16),
                pltpu.VMEM((SLOTS, Q, H), BF16),
                dma((5,)),
                dma((3,)),
                dma((2,)),
                dma((len(STAGES), N)),
                dma((len(STAGES), N)),
                pltpu.SemaphoreType.REGULAR,
            ],
            compiler_params=pltpu.CompilerParams(collective_id=0, has_side_effects=True, vmem_limit_bytes=35 * 2**20),
            cost_estimate=pl.CostEstimate(flops=12 * T * D * F, bytes_accessed=80 * 2**20, transcendentals=T * F),
        )(x, dy, gate, up, w_gate, w_up, w_down)
        return pl.pallas_call(
            store,
            name="store",
            in_specs=[vmem] * 4,
            out_specs=[hbm] * 4,
            out_shape=[jax.ShapeDtypeStruct(h.shape, BF16) for h in held],
            scratch_shapes=[dma((4,))],
            compiler_params=pltpu.CompilerParams(vmem_limit_bytes=2**20),
        )(*held)

    tokens, columns, down = P("dp", None), P(None, "tp"), P("tp", None)
    return jax.shard_map(
        step,
        mesh=mesh,
        in_specs=(tokens, tokens, P("dp", "tp"), P("dp", "tp"), columns, columns, down),
        out_specs=(tokens, P("dp", "tp"), P("dp", "tp"), P(("dp", "tp"), None)),
        check_vma=False,
    )
```

```python
import jax
import jax.numpy as jnp
from jax import lax
from jax.experimental import pallas as pl
from jax.experimental.pallas import tpu as pltpu
from jax.sharding import PartitionSpec as P

MESH = pl.DeviceIdType.MESH
BF16, F32 = jnp.bfloat16, jnp.float32
SQRT_2_OVER_PI = 0.7978845608028654
CUBIC = 0.044715

T, D, F = 2048, 2560, 1280
N = 8
R = T // N
S = R // 2
Q = R // 4
H = D // 2
NT = 256
PIECES = 4
SLOTS = 4
STAGES = ("pair", "a", "b", "c", "own", "fwd", "e1", "e2")

TICKS = {
    "a": (0, 4, 11, 12, 18, 22, 28, 31),
    "b": (3, 8, 15, 17, 23, 27, 31, 34),
    "c": (6, 11, 20, 21, 29, 34, 35, 36),
    "d": (11, 20, 31, 34, 36, 43, 46, 47),
}


def dot_nt(a, b):
    return lax.dot_general(a, b, (((1,), (1,)), ((), ())), preferred_element_type=F32)


def kernel(x, dy, gate, up, wg, wu, wd, dx, dwg, dwu, dwd, dg, du, ht, dyb, xt, acc, pair_in, a_in, b_in, pair_out, a_out, b_out, w_sem, in_sem, x_sem, send_sem, recv_sem, free_sem):
    me = lax.axis_index("tp")
    core = lax.rem(me, 2)
    px, py = me // 4, lax.rem(me // 2, 2)
    p = jnp.where(core == 0, px, py)
    s = jnp.where(core == 0, py, px)
    over_x = (1 - px) * 4 + py * 2 + core
    over_y = px * 4 + (1 - py) * 2 + core
    n1 = jnp.where(core == 0, over_x, over_y)
    n2 = jnp.where(core == 0, over_y, over_x)
    partner = px * 4 + py * 2 + (1 - core)

    mine = pl.ds(pl.multiple_of(core * H, H), H)

    def rows(j, start, size):
        return pl.ds(pl.multiple_of(j * R + start, Q), size)

    def remote(stage, j, src, dst, to):
        k = STAGES.index(stage)
        return pltpu.make_async_remote_copy(src, dst, send_sem.at[k, j], recv_sem.at[k, j], device_id={"tp": to}, device_id_type=MESH)

    def copy_of(stage, j):
        if stage == "pair":
            return remote(stage, j, pair_out.at[lax.rem(j, 2)], pair_in.at[lax.rem(j, 2)], partner)
        if stage == "a":
            return remote(stage, j, a_out.at[lax.rem(j, SLOTS)], a_in.at[lax.rem(j, SLOTS)], n1)
        if stage == "b":
            return remote(stage, j, b_out.at[lax.rem(j, SLOTS)], b_in.at[j], n2)
        if stage == "c":
            at = dx.at[rows(j, S * p + Q * s, Q), mine]
            return remote(stage, j, at, at, n2)
        if stage == "own":
            at = dx.at[rows(j, S * p + Q * s, Q), mine]
            return remote(stage, j, at, at, n1)
        if stage == "fwd":
            at = dx.at[rows(j, S * p + Q * (1 - s), Q), mine]
            return remote(stage, j, at, at, n1)
        at = dx.at[rows(j, S * p if stage == "e1" else S * (1 - p), S), mine]
        return remote(stage, j, at, at, partner)

    def reuse(stage, j, slots):
        @pl.when(j >= slots)
        def _():
            copy_of(stage, j - slots).wait_send()

    def take_a(j):
        copy_of("a", j).wait_recv()
        reuse("b", j, SLOTS)
        k = lax.rem(j, SLOTS)
        keep, leave = pl.ds(pl.multiple_of(Q * s, Q), Q), pl.ds(pl.multiple_of(Q * (1 - s), Q), Q)
        b_out[k] = (acc[k, leave, :] + a_in[k, leave, :].astype(F32)).astype(BF16)
        copy_of("b", j).start()
        acc[k, keep, :] = acc[k, keep, :] + a_in[k, keep, :].astype(F32)

        @pl.when(j + SLOTS < N)
        def _():
            pl.semaphore_signal(free_sem, inc=1, device_id={"tp": n1}, device_id_type=MESH)

    def take_b(j):
        copy_of("b", j).wait_recv()
        keep = pl.ds(pl.multiple_of(Q * s, Q), Q)
        dx[rows(j, S * p + Q * s, Q), mine] = (acc[lax.rem(j, SLOTS), keep, :] + b_in[j].astype(F32)).astype(BF16)
        copy_of("c", j).start()
        copy_of("own", j).start()

    def take_c(j):
        copy_of("c", j).wait_recv()
        copy_of("fwd", j).start()
        copy_of("e1", j).start()

    def take_d(j):
        copy_of("own", j).wait_recv()
        copy_of("fwd", j).wait_recv()
        copy_of("e2", j).start()

    def tick(t, first, last):
        for name, take in (("a", take_a), ("b", take_b), ("c", take_c), ("d", take_d)):
            due = [(j, at) for j, at in enumerate(TICKS[name]) if first <= at <= last]
            if due:
                hit = sum((t == at).astype(jnp.int32) for _, at in due)
                j = sum((t == at).astype(jnp.int32) * j for j, at in due)

                @pl.when(hit > 0)
                def _(take=take, j=j):
                    take(j)

    def local(src, dst, sem):
        return pltpu.make_async_copy(src, dst, sem)

    def inputs(i):
        at = pl.ds(pl.multiple_of(i * R, R), R)
        return (
            local(dy.at[at], dyb, in_sem.at[0]),
            local(gate.at[at], dg.at[at], in_sem.at[1]),
            local(up.at[at], du.at[at], in_sem.at[2]),
        )

    def half(k):
        at = pl.ds(pl.multiple_of((1 - core if k == 0 else core) * H, H), H)
        return local(wg.at[at], dwg.at[at], w_sem.at[2 * k]), local(wu.at[at], dwu.at[at], w_sem.at[2 * k + 1])

    down_weight = local(wd, dwd, w_sem.at[4])
    down_weight.start()
    for c in (*inputs(0), *half(0), *half(1)):
        c.start()

    barrier = pltpu.get_barrier_semaphore()
    for other in (n1, n2, partner):
        pl.semaphore_signal(barrier, inc=1, device_id={"tp": other}, device_id_type=MESH)

    def hidden_part(i):
        at = pl.ds(pl.multiple_of(i * R, R), R)
        dyv = dyb[...]
        for n in range(F // NT):
            cols = pl.ds(n * NT, NT)
            d_hidden = dot_nt(dyv, dwd[cols, :])
            g, u = dg[at, cols].astype(F32), du[at, cols].astype(F32)
            g2 = g * g
            h = 0.5 + 0.5 * jnp.tanh(g * (SQRT_2_OVER_PI + (SQRT_2_OVER_PI * CUBIC) * g2))
            a = g * h
            slope = h + (g * (h - h * h)) * (2 * SQRT_2_OVER_PI + (6 * SQRT_2_OVER_PI * CUBIC) * g2)
            dg[at, cols] = ((d_hidden * u) * slope).astype(BF16)
            du[at, cols] = (d_hidden * a).astype(BF16)
            ht[cols, at] = (a * u).astype(BF16).T

    def term(j, n, col0):
        at = pl.ds(pl.multiple_of(j * R, R), R)
        w = pl.ds(pl.multiple_of(col0 + n * NT, NT), NT)
        d = jnp.concatenate([dg[at, :], du[at, :]], axis=1)
        return dot_nt(d, jnp.concatenate([dwg[w, :], dwu[w, :]], axis=1))

    def pair_part(j):
        reuse("pair", j, 2)
        slot = lax.rem(j, 2)
        for n in range(H // NT):
            pair_out[slot, :, pl.ds(n * NT, NT)] = term(j, n, (1 - core) * H).astype(BF16)
        copy_of("pair", j).start()

    def own_ready(j):
        copy_of("pair", j).wait_recv()
        reuse("a", j, SLOTS)

        @pl.when(j >= SLOTS)
        def _():
            pl.semaphore_wait(free_sem, 1)

    def own_part(j):
        slot, k = lax.rem(j, 2), lax.rem(j, SLOTS)
        for n in range(H // NT):
            cols = pl.ds(n * NT, NT)
            total = term(j, n, core * H) + pair_in[slot, :, cols].astype(F32)
            lo, hi = total[:S], total[S:]
            acc[k, :, cols] = jnp.where(p == 0, lo, hi)
            a_out[k, :, cols] = jnp.where(p == 0, hi, lo).astype(BF16)
        copy_of("a", j).start()

    def wait_inputs(i):
        for c in inputs(i):
            c.wait()

    def next_inputs(i):
        @pl.when(i < N)
        def _():
            for c in inputs(i):
                c.start()

    zero, one = jnp.int32(0), jnp.int32(1)

    def part(f, j):
        @pl.when(me >= 0)
        def _():
            f(j)

    wait_inputs(zero)
    down_weight.wait()
    part(hidden_part, zero)
    next_inputs(one)
    for c in half(0):
        c.wait()
    pl.semaphore_wait(barrier, 3)
    part(pair_part, zero)
    for c in half(1):
        c.wait()
    own_ready(zero)
    part(own_part, zero)
    wait_inputs(one)
    part(hidden_part, one)
    next_inputs(one + 1)
    part(pair_part, one)
    LAST = 3 * N - 7

    def chunk(i, _):
        wait_inputs(i)
        hidden_part(i)
        next_inputs(i + 1)
        tick(3 * i - 6, 0, LAST)
        own_ready(i - 1)

        @pl.when(i > 1)
        def _():
            own_part(i - 1)

        tick(3 * i - 5, 0, LAST)
        pair_part(i)
        tick(3 * i - 4, 0, LAST)
        return ()

    lax.fori_loop(2, N, chunk, ())

    def tile(src, n):
        slot = lax.rem(n, 2)
        return local(src.at[:, pl.ds(pl.multiple_of(n * NT, NT), NT)], xt.at[slot], x_sem.at[slot])

    TILES = D // NT
    tile(dy, 0).start()
    own_ready(jnp.int32(N - 1))
    own_part(jnp.int32(N - 1))
    t0 = LAST + 1
    tick(jnp.int32(t0), t0, t0)
    t0 += 1

    def down(n, _):
        tile(dy, n).wait()

        @pl.when(n + 1 < TILES)
        def _():
            tile(dy, n + 1).start()

        @pl.when(n + 1 == TILES)
        def _():
            tile(x, zero).start()

        cols = pl.ds(pl.multiple_of(n * NT, NT), NT)
        dwd[:, cols] = jnp.dot(ht[...], xt[lax.rem(n, 2)], preferred_element_type=F32).astype(BF16)
        tick(t0 + n, t0, t0 + TILES - 1)
        return ()

    lax.fori_loop(0, TILES, down, ())
    t1 = t0 + TILES

    def turn(n):
        ht[pl.ds(pl.multiple_of(lax.rem(n, 2) * NT, NT), NT), :] = xt[lax.rem(n, 2)].T

    tile(x, zero).wait()
    tile(x, one).start()
    turn(zero)

    def gate_up(n, _):
        @pl.when(n + 1 < TILES)
        def _():
            tile(x, n + 1).wait()

        @pl.when(n + 2 < TILES)
        def _():
            tile(x, n + 2).start()

        at = pl.ds(pl.multiple_of(n * NT, NT), NT)
        xv = ht[pl.ds(pl.multiple_of(lax.rem(n, 2) * NT, NT), NT), :]
        dwg[at, :] = jnp.dot(xv, dg[...], preferred_element_type=F32).astype(BF16)
        turn(n + 1)
        dwu[at, :] = jnp.dot(xv, du[...], preferred_element_type=F32).astype(BF16)
        tick(t1 + n, t1, t1 + TILES - 1)
        return ()

    lax.fori_loop(0, TILES, gate_up, ())

    t2 = t1 + TILES

    def drain(t, _):
        tick(t, t2, 99)
        return ()

    lax.fori_loop(t2, max(TICKS["d"]) + 1, drain, ())

    def finish(j, _):
        copy_of("e1", j).wait_recv()
        copy_of("e2", j).wait_recv()
        for stage in STAGES[3:]:
            copy_of(stage, j).wait_send()
        for stage, slots in (("pair", 2), ("a", SLOTS), ("b", SLOTS)):

            @pl.when(j >= N - slots)
            def _(stage=stage):
                copy_of(stage, j).wait_send()

        return ()

    lax.fori_loop(0, N, finish, ())


def store(*refs):
    n = (len(refs) - 1) // 2
    copies = []
    for part in range(PIECES):
        for k in range(n):
            size = refs[k].shape[0] // PIECES
            at = pl.ds(part * size, size)
            copies.append(pltpu.make_async_copy(refs[k].at[at], refs[n + k].at[at], refs[-1].at[k, part]))
    for c in copies:
        c.start()
    for c in copies:
        c.wait()


def solution(mesh):
    def step(x, dy, gate, up, w_gate, w_up, w_down):
        hbm = pl.BlockSpec(memory_space=pltpu.HBM)
        vmem = pl.BlockSpec(memory_space=pltpu.VMEM)
        dma = pltpu.SemaphoreType.DMA
        held = pl.pallas_call(
            kernel,
            name="mlp_backward",
            in_specs=[hbm] * 7,
            out_specs=[vmem] * 4,
            out_shape=[pltpu.VMEM((T, D), BF16), pltpu.VMEM((D, F), BF16), pltpu.VMEM((D, F), BF16), pltpu.VMEM((F, D), BF16)],
            scratch_shapes=[
                pltpu.VMEM((T, F), BF16),
                pltpu.VMEM((T, F), BF16),
                pltpu.VMEM((F, T), BF16),
                pltpu.VMEM((R, D), BF16),
                pltpu.VMEM((2, T, NT), BF16),
                pltpu.VMEM((SLOTS, S, H), F32),
                pltpu.VMEM((2, R, H), BF16),
                pltpu.VMEM((SLOTS, S, H), BF16),
                pltpu.VMEM((N, Q, H), BF16),
                pltpu.VMEM((2, R, H), BF16),
                pltpu.VMEM((SLOTS, S, H), BF16),
                pltpu.VMEM((SLOTS, Q, H), BF16),
                dma((5,)),
                dma((3,)),
                dma((2,)),
                dma((len(STAGES), N)),
                dma((len(STAGES), N)),
                pltpu.SemaphoreType.REGULAR,
            ],
            compiler_params=pltpu.CompilerParams(collective_id=0, has_side_effects=True, vmem_limit_bytes=35 * 2**20),
            cost_estimate=pl.CostEstimate(flops=12 * T * D * F, bytes_accessed=80 * 2**20, transcendentals=T * F),
        )(x, dy, gate, up, w_gate, w_up, w_down)
        return pl.pallas_call(
            store,
            name="store",
            in_specs=[vmem] * 4,
            out_specs=[hbm] * 4,
            out_shape=[jax.ShapeDtypeStruct(h.shape, BF16) for h in held],
            scratch_shapes=[dma((4, PIECES))],
            compiler_params=pltpu.CompilerParams(vmem_limit_bytes=2**20),
        )(*held)

    tokens, columns, down = P("dp", None), P(None, "tp"), P("tp", None)
    return jax.shard_map(
        step,
        mesh=mesh,
        in_specs=(tokens, tokens, P("dp", "tp"), P("dp", "tp"), columns, columns, down),
        out_specs=(tokens, P("dp", "tp"), P("dp", "tp"), P(("dp", "tp"), None)),
        check_vma=False,
    )
```
